256 devices in a mesh: gx: 32 (over z, x_hi, core), gy: 8 (over x_lo, y).
Axes of the slice: x: 4 (x_hi: 2, x_lo: 2; x = x_hi * 2 + x_lo), y: 4, z: 8, core: 2. Of those that a mesh axis runs over, the one named last changes fastest.
Arguments:
- positions: float32 [3, 12, 64, 128, 256], P(None, None, 'gx', 'gy'), may hold values from 0 to 1
- velocities: float32 [3, 12, 64, 128, 256], P(None, None, 'gx', 'gy'), may hold values from -6 to 6
- thermal: float32 [3, 12, 64, 128, 256], P(None, None, 'gx', 'gy'), may hold values from -6 to 6
- offsets: int32 [12, 64, 128, 256], P(None, 'gx', 'gy'), may hold values from 0 to 7
- occupancy: int32 [12, 64, 128, 256], P(None, 'gx', 'gy'), may hold values from 0 to 1, as said below
- shift_codes: int32 [3], replicated, may hold values from 0 to 7
Outputs:
- new_velocities: float32 [3, 12, 64, 128, 256], P(None, None, 'gx', 'gy')
The draws below stay inside these ranges and needn't reach their ends.
Inputs may be any that keep to these rules, and one draw needn't show every extreme that they name: `occupancy`: the particles of a storage cell occupy its first slots; every storage cell holds 8 to 12 particles.
All inputs are finite; a program needn't handle non-finite values.
Results may differ from the reference program's by a relative error of at most 0.0001.
Values sent between devices are 32-bit elements; how exact they have to be, the bound alone decides.
A program may use at most 64 MiB of HBM per device.

```python
import jax
import jax.numpy as jnp

CZ = 256
SLOTS = 12
STEPS = 3
NX = 64
NY = 128


def draw_occupancy(key, part):
    counts = jax.random.randint(key, (1, NX, NY, CZ), SLOTS - 4, SLOTS + 1)
    slot_ids = jnp.arange(SLOTS, dtype=jnp.int32).reshape(SLOTS, 1, 1, 1)
    return (slot_ids < counts).astype(jnp.int32)


def touch_ends(drawn, own_key, least, largest):
    longest = drawn.shape.index(max(drawn.shape))
    spots = []
    for shift in (0, 1):
        where = [jax.random.randint(jax.random.fold_in(own_key, axis), (), 0, length) for axis, length in enumerate(drawn.shape)]
        where[longest] = (where[longest] + shift) % drawn.shape[longest]
        spots.append(tuple(where))
    return drawn.at[spots[0]].set(least).at[spots[1]].set(largest)


def levels(key, shape, cuts, least, largest):
    gain = 1.0
    for axis_at, blocks in cuts:
        draws = jax.random.uniform(jax.random.fold_in(jax.random.fold_in(key, 6), axis_at), (blocks,), jnp.float32, least / len(cuts), largest / len(cuts))
        gain = gain * jnp.repeat(jnp.exp(draws), shape[axis_at] // blocks).reshape((-1,) + (1,) * (len(shape) - 1 - axis_at))
    return gain


def bell_draw(own_key, extent, scale, reach, cuts=(), kind=jnp.bfloat16):
    gain = levels(own_key, extent, cuts, -0.22, 0.18) if cuts else 1.0
    drawn = jax.random.normal(own_key, extent, jnp.float32) * scale * gain
    return jnp.minimum(jnp.maximum(drawn, -reach), reach).astype(kind)


def setup_inputs(seed: int = 0) -> dict:
    splits = jax.random.split(jax.random.key(seed), 7)
    positions = jnp.clip(1.0 * jax.random.uniform(splits[0], (3, SLOTS, NX, NY, CZ), jnp.float32) ** levels(splits[0], (3, SLOTS, NX, NY, CZ), ((2, 32), (3, 8)), -0.2, 0.2), 0.0, 1.0)
    velocities = bell_draw(splits[1], (3, SLOTS, NX, NY, CZ), 1.0, 6.0, ((2, 32), (3, 8)), jnp.float32)
    thermal = bell_draw(splits[2], (3, SLOTS, NX, NY, CZ), 1.0, 6.0, ((2, 32), (3, 8)), jnp.float32)
    offsets = touch_ends(jax.random.randint(splits[3], (SLOTS, NX, NY, CZ), 0, 8), jax.random.fold_in(splits[3], 1), 0, 7).astype(jnp.int32)
    occupancy = draw_occupancy(jax.random.fold_in(splits[6], 71), 0)
    shift_codes = jax.random.randint(splits[5], (STEPS,), 0, 8).astype(jnp.int32)
    return dict(positions=positions, velocities=velocities, thermal=thermal, offsets=offsets, occupancy=occupancy, shift_codes=shift_codes)


ridge = 0.5


def offset_bits(code_value):
    return code_value // 4, (code_value // 2) % 2, code_value % 2


def cross_product(first, second):
    return [first[1] * second[2] - first[2] * second[1],
            first[2] * second[0] - first[0] * second[2],
            first[0] * second[1] - first[1] * second[0]]


def code_moments(positions, velocities, thermal, offsets, occupancy, code_value):
    shift_x, shift_y, shift_z = offset_bits(code_value)
    weight = jnp.where(offsets == code_value, occupancy, 0).astype(jnp.float32)
    shifted = [positions[0] + shift_x, positions[1] + shift_y, positions[2] + shift_z]
    relative = [velocities[component] - thermal[component] for component in range(3)]
    spins = cross_product(shifted, relative)
    seconds = [shifted[0] * shifted[0], shifted[1] * shifted[1], shifted[2] * shifted[2],
               shifted[0] * shifted[1], shifted[0] * shifted[2], shifted[1] * shifted[2]]
    terms = shifted + relative + spins + seconds
    return jnp.stack([jnp.sum(weight, axis=0)] + [jnp.sum(weight * term, axis=0) for term in terms])


def cell_solution(sums):
    count = jnp.maximum(sums[0], 1.0)
    first = [sums[1], sums[2], sums[3]]
    flow = [sums[4], sums[5], sums[6]]
    centre = [value / count for value in first]
    drift = [value / count for value in flow]
    moment = cross_product(centre, flow)
    torque = [sums[7 + component] - moment[component] for component in range(3)]
    mxx = sums[10] - first[0] * first[0] / count
    myy = sums[11] - first[1] * first[1] / count
    mzz = sums[12] - first[2] * first[2] / count
    mxy = sums[13] - first[0] * first[1] / count
    mxz = sums[14] - first[0] * first[2] / count
    myz = sums[15] - first[1] * first[2] / count
    trace = mxx + myy + mzz
    kxx = trace - mxx + ridge
    kyy = trace - myy + ridge
    kzz = trace - mzz + ridge
    kxy = -mxy
    kxz = -mxz
    kyz = -myz
    adj_xx = kyy * kzz - kyz * kyz
    adj_yy = kxx * kzz - kxz * kxz
    adj_zz = kxx * kyy - kxy * kxy
    adj_xy = kxz * kyz - kxy * kzz
    adj_xz = kxy * kyz - kxz * kyy
    adj_yz = kxy * kxz - kxx * kyz
    determinant = kxx * adj_xx + kxy * adj_xy + kxz * adj_xz
    spin_x = (adj_xx * torque[0] + adj_xy * torque[1] + adj_xz * torque[2]) / determinant
    spin_y = (adj_xy * torque[0] + adj_yy * torque[1] + adj_yz * torque[2]) / determinant
    spin_z = (adj_xz * torque[0] + adj_yz * torque[1] + adj_zz * torque[2]) / determinant
    return jnp.stack(centre + drift + [spin_x, spin_y, spin_z])


def particle_update(table, positions, thermal, offsets, occupancy, code_value, total):
    shift_x, shift_y, shift_z = offset_bits(code_value)
    shifted = [positions[0] + shift_x, positions[1] + shift_y, positions[2] + shift_z]
    arm = [shifted[component] - table[component] for component in range(3)]
    turn = cross_product([table[6], table[7], table[8]], arm)
    fresh = jnp.stack([thermal[component] + table[3 + component] + turn[component] for component in range(3)])
    keep = (offsets == code_value) & (occupancy == 1)
    return total + jnp.where(keep, fresh, jnp.zeros_like(fresh))


def one_collision(positions, velocities, thermal, offsets, occupancy):
    cell_sums = jnp.zeros((16,) + offsets.shape[1:], jnp.float32)
    for code_value in range(8):
        shift_x, shift_y, shift_z = offset_bits(code_value)
        partial_sums = code_moments(positions, velocities, thermal, offsets, occupancy, code_value)
        cell_sums = cell_sums + jnp.roll(partial_sums, (-shift_x, -shift_y, -shift_z), axis=(1, 2, 3))
    state = cell_solution(cell_sums)
    result = jnp.zeros(positions.shape, jnp.float32)
    for code_value in range(8):
        shift_x, shift_y, shift_z = offset_bits(code_value)
        table = jnp.roll(state, (shift_x, shift_y, shift_z), axis=(1, 2, 3))
        result = particle_update(table, positions, thermal, offsets, occupancy, code_value, result)
    return result


def reference(positions, velocities, thermal, offsets, occupancy, shift_codes):
    current = velocities
    for step_index in range(STEPS):
        codes = jnp.bitwise_xor(offsets, shift_codes[step_index])
        hot = jnp.roll(thermal, -step_index, axis=1)
        current = one_collision(positions, current, hot, codes, occupancy)
    return current
```

```python
import functools

import jax
import jax.numpy as jnp
from jax import lax
from jax.experimental import pallas as pl
from jax.experimental.pallas import tpu as pltpu
from jax.sharding import PartitionSpec as P

MESH = pl.DeviceIdType.MESH
f32 = jnp.float32
SLOTS = 12
ridge = 0.5

O, M, I = 0, 1, 2
ROW_PARTS = {O: ((0, 1),), M: ((0, 0), (1, 0)), I: ((1, 1),)}
STATIC, DYNAMIC = 10, 6
FIELDS = (STATIC, DYNAMIC) * 3
XMSG = ("bulk", "edge", "dup", "ddown")


def kernel(
    shift_ref, pos_h, vel_h, th_h, off_h, occ_h, out_ref,
    pos, vel, th, off, occ, code, gs, gd, wb,
    es0, ed0, es1, ed1, es2, ed2,
    rb0, rb1, rb2, rb3, rb4, rb5,
    sd, su, sdz, ru, rd, rxe, rxu, rxd, cm, ct, op, ope, tm, te, tr,
    in_sem, out_sem, s_sem, r_sem,
):
    es, ed = (es0, es1, es2), (ed0, ed1, ed2)
    e = (es0, ed0, es1, ed1, es2, ed2)
    rb = (rb0, rb1, rb2, rb3, rb4, rb5)
    gx, gy = lax.axis_index("gx"), lax.axis_index("gy")
    ngx, ngy = lax.axis_size("gx"), lax.axis_size("gy")
    core = lax.rem(gx, 2)
    off_gx = lax.rem(gx + 2 * core - 1 + ngx, ngx)
    on_gx = gx + 1 - 2 * core
    up, down = lax.rem(gy + 1, ngy), lax.rem(gy + ngy - 1, ngy)
    rows = (core, 1 - core)
    sh = [shift_ref[0], shift_ref[1], shift_ref[2]]

    copies = []
    for r in (0, 1):
        for t, (src, dst) in enumerate(((off_h, off), (occ_h, occ), (pos_h, pos), (th_h, th), (vel_h, vel))):
            view = src.at[:, rows[r]] if t < 2 else src.at[:, :, rows[r]]
            c = pltpu.make_async_copy(view, dst.at[r], in_sem.at[r, t])
            c.start()
            copies.append(c)

    barrier = pltpu.get_barrier_semaphore()
    for to in ((off_gx, gy), (on_gx, gy), (gx, up), (gx, down), (off_gx, up), (off_gx, down), (on_gx, up), (on_gx, down)):
        pl.semaphore_signal(barrier, inc=1, device_id=to, device_id_type=MESH)

    core_f = core.astype(f32)
    xbit = {(0, 1): 1.0 - core_f, (0, 0): core_f, (1, 1): core_f, (1, 0): 1.0 - core_f}
    flip = (core * 4, (1 - core) * 4)

    def chunked(body):
        def step(t, carry):
            ys = pl.ds(pl.multiple_of(8 * (t // 2), 8), 8)
            zs = pl.ds(pl.multiple_of(128 * lax.rem(t, 2), 128), 128)
            body(ys, zs)
            return carry
        lax.fori_loop(0, 4, step, 0)

    def make_codes(r):
        x = sh[0] ^ flip[r]
        for m in range(SLOTS):
            code[r, m] = jnp.where(occ[r, m] == 1, off[r, m] ^ x, 8)

    def accumulate(acc, mask, vals):
        for f, v in enumerate(vals):
            term = jnp.where(mask, v, 0.0)
            acc[f] = term if acc[f] is None else acc[f] + term

    def static_moments(r, p):
        def body(ys, zs):
            acc = [[None] * STATIC for _ in range(4)]
            for m in range(SLOTS):
                k = code[r, m, ys, zs]
                x, y, z = (pos[r, a, m, ys, zs] for a in range(3))
                vals = [1.0, x, y, z, x * x, y * y, z * z, x * y, x * z, y * z]
                for q in range(4):
                    accumulate(acc[q], k == p * 4 + q, vals)
            for q in range(4):
                for f in range(STATIC):
                    gs[r, p * 4 + q, f, ys, zs] = acc[q][f]
        chunked(body)

    def dynamic_moments(s, r, p):
        def body(ys, zs):
            acc = [[None] * DYNAMIC for _ in range(4)]
            for m in range(SLOTS):
                k = code[r, m, ys, zs]
                x, y, z = (pos[r, a, m, ys, zs] for a in range(3))
                if s == 0:
                    w = [vel[r, a, m, ys, zs] - th[r, a, m, ys, zs] for a in range(3)]
                else:
                    w = [th[r, a, (m + s - 1) % SLOTS, ys, zs] - th[r, a, (m + s) % SLOTS, ys, zs] for a in range(3)]
                vals = w + [y * w[2] - z * w[1], z * w[0] - x * w[2], x * w[1] - y * w[0]]
                for q in range(4):
                    accumulate(acc[q], k == p * 4 + q, vals)
            for q in range(4):
                for f in range(DYNAMIC):
                    gd[s, r, p * 4 + q, f, ys, zs] = acc[q][f]
        chunked(body)

    def static_field(load, f, bx, by, bz):
        v = load(f)
        if f == 1:
            v = v + bx * load(0)
        elif f == 2 and by:
            v = v + load(0)
        elif f == 3 and bz:
            v = v + load(0)
        elif f == 4:
            v = v + bx * (2.0 * load(1) + load(0))
        elif f == 5 and by:
            v = v + (2.0 * load(2) + load(0))
        elif f == 6 and bz:
            v = v + (2.0 * load(3) + load(0))
        elif f == 7:
            v = v + bx * (load(2) + load(0) if by else load(2))
            v = v + load(1) if by else v
        elif f == 8:
            v = v + bx * (load(3) + load(0) if bz else load(3))
            v = v + load(1) if bz else v
        elif f == 9:
            if by:
                v = v + load(3)
            if bz:
                v = v + load(2)
            if by and bz:
                v = v + load(0)
        return v

    def dynamic_field(load, f, bx, by, bz):
        v = load(f)
        if f == 3:
            v = v + load(2) if by else v
            v = v - load(1) if bz else v
        elif f == 4:
            v = v - bx * load(2)
            v = v + load(0) if bz else v
        elif f == 5:
            v = v + bx * load(1)
            v = v - load(0) if by else v
        return v

    not_last = lax.broadcasted_iota(jnp.int32, (16, 256), 0) < 15
    is_last = lax.broadcasted_iota(jnp.int32, (16, 256), 0) == 15
    is_first = lax.broadcasted_iota(jnp.int32, (16, 256), 0) == 0

    def assemble(ph, row, source, field):
        n = FIELDS[ph]
        for f in range(n):
            planes = []
            for bz in (0, 1):
                total = [None, None]
                for by in (0, 1):
                    for r, p in ROW_PARTS[row]:
                        load = functools.partial(source, r, p * 4 + by * 2 + bz)
                        v = field(load, f, xbit[r, p], by, bz)
                        total[by] = v if total[by] is None else total[by] + v
                sdz[bz, f : f + 1] = total[1][0:1]
                planes.append(total[0] + jnp.where(not_last, pltpu.roll(total[1], 15, 0), 0.0))
            whole = planes[0] + pltpu.roll(planes[1], 255, 1)
            e[ph][row, f] = whole
            su[ph, row, f : f + 1] = whole[15:16]
        sd[ph, row] = sdz[0] + pltpu.roll(sdz[1], 255, 1)

    def remote(ph, j, src, dst, to):
        return pltpu.make_async_remote_copy(
            src_ref=src, dst_ref=dst, send_sem=s_sem.at[ph, j], recv_sem=r_sem.at[ph, j], device_id=to, device_id_type=MESH
        )

    def messages(ph, row):
        n = 16 if ph == -1 else FIELDS[ph]
        fs = pl.ds(0, 8 if n <= 8 else 16)
        low, high = sd.at[ph, row, fs], su.at[ph, row, fs]
        out = [
            remote(ph, 8 + 2 * row, low, ru.at[ph, row, fs], (gx, down)),
            remote(ph, 9 + 2 * row, high, rd.at[ph, row, fs], (gx, up)),
        ]
        if row != M:
            side = 0 if row == O else 1
            to = off_gx if row == O else on_gx
            out += [
                remote(ph, 4 * side + 2, low, rxu.at[ph, side, fs], (to, down)),
                remote(ph, 4 * side + 3, high, rxd.at[ph, side, fs], (to, up)),
                remote(ph, 4 * side + 1, low, rxe.at[ph, side, fs], (to, gy)),
                remote(ph, 4 * side, e[ph].at[row], rb[ph].at[side], (to, gy)),
            ]
        return out

    def send(ph, row):
        for c in messages(ph, row):
            c.start()

    def receive(ph, row):
        for c in messages(ph, row):
            c.wait_recv()

    def totals(ph, row):
        low, high = sd[ph, row] + rd[ph, row], ru[ph, row]
        if row != M:
            side = 0 if row == O else 1
            low = low + rxe[ph, side] + rxd[ph, side]
            high = high + rxu[ph, side]
        cm[ph, row] = low
        ct[ph, row] = high

    def total(ph, row, f):
        v = e[ph][row, f]
        if row != M:
            v = v + rb[ph][0 if row == O else 1, f]
        return v + jnp.where(is_last, ct[ph, row, f : f + 1], 0.0)

    def invert(a):
        n, sx, sy, sz, xx, yy, zz, xy, xz, yz = a
        inv = 1.0 / jnp.maximum(n, 1.0)
        cx, cy, cz = sx * inv, sy * inv, sz * inv
        mxx, myy, mzz = xx - sx * cx, yy - sy * cy, zz - sz * cz
        kxy, kxz, kyz = sx * cy - xy, sx * cz - xz, sy * cz - yz
        kxx, kyy, kzz = myy + mzz + ridge, mxx + mzz + ridge, mxx + myy + ridge
        axx = kyy * kzz - kyz * kyz
        ayy = kxx * kzz - kxz * kxz
        azz = kxx * kyy - kxy * kxy
        axy = kxz * kyz - kxy * kzz
        axz = kxy * kyz - kxz * kyy
        ayz = kxy * kxz - kxx * kyz
        idet = 1.0 / (kxx * axx + kxy * axy + kxz * axz)
        return [inv, cx, cy, cz, axx * idet, ayy * idet, azz * idet, axy * idet, axz * idet, ayz * idet]

    def respond(o, d):
        inv, cx, cy, cz, axx, ayy, azz, axy, axz, ayz = o
        wx, wy, wz, lx, ly, lz = d
        tx, ty, tz = lx - (cy * wz - cz * wy), ly - (cz * wx - cx * wz), lz - (cx * wy - cy * wx)
        ox = axx * tx + axy * ty + axz * tz
        oy = axy * tx + ayy * ty + ayz * tz
        oz = axz * tx + ayz * ty + azz * tz
        return [wx * inv - (oy * cz - oz * cy), wy * inv - (oz * cx - ox * cz), wz * inv - (ox * cy - oy * cx), ox, oy, oz]

    def static_solve(s, row):
        for f, v in enumerate(invert([total(2 * s, row, f) for f in range(STATIC)])):
            op[row, f] = v
        o = invert([cm[2 * s, row, f : f + 1] for f in range(STATIC)])
        for f, v in enumerate(o):
            ope[row, f : f + 1] = v

    def dynamic_solve(s, row):
        ph = 2 * s + 1
        t = respond([op[row, f] for f in range(STATIC)], [total(ph, row, f) for f in range(DYNAMIC)])
        x = respond([ope[row, f : f + 1] for f in range(STATIC)], [cm[ph, row, f : f + 1] for f in range(DYNAMIC)])
        for f in range(DYNAMIC):
            te[row, f : f + 1] = x[f]
            tm[row, f] = t[f]
        te[row, 8:16] = pltpu.roll(te[row, 0:8], 1, 1)
        for f in range(DYNAMIC):
            v = tm[row, f]
            for bz in (0, 1):
                v = v if bz == 0 else pltpu.roll(v, 1, 1)
                tr[row, bz, f] = v
                tr[row, 2 + bz, f] = jnp.where(is_first, te[row, 8 * bz + f : 8 * bz + f + 1], pltpu.roll(v, 1, 0))

    def offset(t, bx, by, bz):
        ax, ay, az, ox, oy, oz = t
        if bz:
            ax, ay = ax + oy, ay - ox
        if by:
            ax, az = ax - oz, az + ox
        return [ax, ay + bx * oz, az - bx * oy, ox, oy, oz]

    def advance(s, r):
        delta = sh[0] ^ sh[s - 1]
        for p in (0, 1):
            row = M if p == 0 else (O if r == 0 else I)
            for q in range(4):
                g = p * 4 + q
                src = g if s == 1 else g ^ delta
                for h in (0, 1):
                    ys = pl.ds(8 * h, 8)
                    t = [tr[row, q, f, ys] for f in range(6)]
                    ax, ay, az, ox, oy, oz = offset(t, xbit[r, p], q // 2, q % 2)
                    n, x, y, z, xx, yy, zz, xy, xz, yz = (gs[r, src, f, ys] for f in range(STATIC))
                    d = [gd[s, r, src, f, ys] for f in range(6)]
                    wb[s - 1, r, g, 0, ys] = d[0] + n * ax + (oy * z - oz * y)
                    wb[s - 1, r, g, 1, ys] = d[1] + n * ay + (oz * x - ox * z)
                    wb[s - 1, r, g, 2, ys] = d[2] + n * az + (ox * y - oy * x)
                    wb[s - 1, r, g, 3, ys] = d[3] + (y * az - z * ay) + ((yy + zz) * ox - xy * oy - xz * oz)
                    wb[s - 1, r, g, 4, ys] = d[4] + (z * ax - x * az) + ((xx + zz) * oy - xy * ox - yz * oz)
                    wb[s - 1, r, g, 5, ys] = d[5] + (x * ay - y * ax) + ((xx + yy) * oz - xz * ox - yz * oy)

    def static_source(s):
        delta = sh[0] ^ sh[s]
        return lambda r, g, f: gs[r, g if s == 0 else g ^ delta, f]

    def dynamic_source(s):
        if s == 0:
            return lambda r, g, f: gd[0, r, g, f]
        delta = sh[s - 1] ^ sh[s]
        return lambda r, g, f: wb[s - 1, r, g ^ delta, f]

    def finish(r):
        delta = sh[0] ^ sh[2]
        def body(ys, zs):
            tables = []
            for p in (0, 1):
                row = M if p == 0 else (O if r == 0 else I)
                for q in range(4):
                    t = [tr[row, q, f, ys, zs] for f in range(6)]
                    tables.append(offset(t, xbit[r, p], q // 2, q % 2))
            for m in range(SLOTS):
                k = code[r, m, ys, zs] ^ delta
                bz, by, bx = (k & 1) == 1, (k & 2) == 2, (k & 4) == 4
                t = []
                for f in range(6):
                    c = [jnp.where(bz, tables[2 * j + 1][f], tables[2 * j][f]) for j in range(4)]
                    c = [jnp.where(by, c[1], c[0]), jnp.where(by, c[3], c[2])]
                    t.append(jnp.where(bx, c[1], c[0]))
                ax, ay, az, ox, oy, oz = t
                x, y, z = (pos[r, a, m, ys, zs] for a in range(3))
                hot = [th[r, a, (m + 2) % SLOTS, ys, zs] for a in range(3)]
                live = k < 8
                out_ref[0, m, rows[r], ys, zs] = jnp.where(live, hot[0] + ax + (oy * z - oz * y), 0.0)
                out_ref[1, m, rows[r], ys, zs] = jnp.where(live, hot[1] + ay + (oz * x - ox * z), 0.0)
                out_ref[2, m, rows[r], ys, zs] = jnp.where(live, hot[2] + az + (ox * y - oy * x), 0.0)
        chunked(body)

    sdz[...] = jnp.zeros_like(sdz)
    su[...] = jnp.zeros_like(su)
    te[...] = jnp.zeros_like(te)
    for t in range(5):
        copies[t].wait()
    make_codes(0)
    static_moments(0, 1)
    dynamic_moments(0, 0, 1)
    assemble(0, O, static_source(0), static_field)
    assemble(1, O, dynamic_source(0), dynamic_field)
    pl.semaphore_wait(barrier, 8)
    send(0, O)
    send(1, O)
    static_moments(0, 0)
    assemble(2, O, static_source(1), static_field)
    send(2, O)
    dynamic_moments(0, 0, 0)
    for t in range(5, 10):
        copies[t].wait()
    make_codes(1)
    for p in (0, 1):
        static_moments(1, p)
        dynamic_moments(0, 1, p)
    for row in (M, I):
        assemble(0, row, static_source(0), static_field)
        assemble(1, row, dynamic_source(0), dynamic_field)
        send(0, row)
        send(1, row)
    for row in (M, I):
        assemble(2, row, static_source(1), static_field)
        send(2, row)
    for row in (M, I, O):
        assemble(4, row, static_source(2), static_field)
        if row != O:
            send(4, row)
    for r in (0, 1):
        for p in (0, 1):
            dynamic_moments(1, r, p)
    for s in (0, 1, 2):
        for row in (M, I, O):
            receive(2 * s, row)
            totals(2 * s, row)
            static_solve(s, row)
        for row in (M, I, O):
            receive(2 * s + 1, row)
            totals(2 * s + 1, row)
            dynamic_solve(s, row)
        if s < 2:
            advance(s + 1, 0)
            assemble(2 * s + 3, O, dynamic_source(s + 1), dynamic_field)
            send(2 * s + 3, O)
            if s == 0:
                send(4, O)
            advance(s + 1, 1)
            for row in (M, I):
                assemble(2 * s + 3, row, dynamic_source(s + 1), dynamic_field)
                send(2 * s + 3, row)
            if s == 0:
                for r in (0, 1):
                    for p in (0, 1):
                        dynamic_moments(2, r, p)
    for r in (0, 1):
        finish(r)
    for ph in range(6):
        for row in (O, M, I):
            for c in messages(ph, row):
                c.wait_send()


def local(positions, velocities, thermal, offsets, occupancy, shift_codes):
    any_space = pl.BlockSpec(memory_space=pl.ANY)
    rows = lambda n: pltpu.VMEM((n, 16, 256), f32)
    per = lambda *lead: pltpu.VMEM((*lead, 16, 256), f32)
    return pl.pallas_call(
        kernel,
        out_shape=jax.ShapeDtypeStruct(positions.shape, f32),
        in_specs=[pl.BlockSpec(memory_space=pltpu.SMEM)] + [any_space] * 5,
        out_specs=pl.BlockSpec(memory_space=pltpu.VMEM),
        scratch_shapes=[
            per(2, 3, SLOTS), per(2, 3, SLOTS), per(2, 3, SLOTS),
            pltpu.VMEM((2, SLOTS, 16, 256), jnp.int32), pltpu.VMEM((2, SLOTS, 16, 256), jnp.int32), pltpu.VMEM((2, SLOTS, 16, 256), jnp.int32),
            per(2, 8, STATIC), per(3, 2, 8, DYNAMIC), per(2, 2, 8, DYNAMIC),
            *[per(3, n) for n in FIELDS],
            *[per(2, n) for n in FIELDS],
            per(6, 3), per(6, 3), per(2), per(6, 3), per(6, 3), per(6, 2), per(6, 2), per(6, 2), per(6, 3), per(6, 3),
            per(3, STATIC), per(3), per(3, DYNAMIC), per(3), per(3, 4, DYNAMIC),
            pltpu.SemaphoreType.DMA((2, 5)), pltpu.SemaphoreType.DMA((2,)),
            pltpu.SemaphoreType.DMA((6, 14)), pltpu.SemaphoreType.DMA((6, 14)),
        ],
        compiler_params=pltpu.CompilerParams(collective_id=0, has_side_effects=True),
    )(shift_codes, positions, velocities, thermal, offsets, occupancy)


def solution(mesh):
    in_specs = (
        P(None, None, "gx", "gy", None),
        P(None, None, "gx", "gy", None),
        P(None, None, "gx", "gy", None),
        P(None, "gx", "gy", None),
        P(None, "gx", "gy", None),
        P(),
    )
    out_specs = P(None, None, "gx", "gy", None)
    return jax.shard_map(local, mesh=mesh, in_specs=in_specs, out_specs=out_specs, check_vma=False)
```

```python
import functools

import jax
import jax.numpy as jnp
from jax import lax
from jax.experimental import pallas as pl
from jax.experimental.pallas import tpu as pltpu
from jax.sharding import PartitionSpec as P

MESH = pl.DeviceIdType.MESH
f32 = jnp.float32
SLOTS = 12
ridge = 0.5

O, M, I = 0, 1, 2
ROW_PARTS = {O: ((0, 1),), M: ((0, 0), (1, 0)), I: ((1, 1),)}
STATIC, DYNAMIC = 10, 6
FIELDS = (STATIC, DYNAMIC) * 3
A, B, C, D = 0, 1, 2, 3
GROUP = (A, A, B, C, B, D)
BASE = (0, STATIC, 0, 0, STATIC, 0)
SPAN = (16, 24, 8, 8)


def kernel(
    shift_h, pos_h, vel_h, th_h, off_h, occ_h, out_ref,
    pos, vel, th, off, occ, code, gs, gd, wb,
    es0, ed0, es1, ed1, es2, ed2,
    rb0, rb1, rb2, rb3, rb4, rb5,
    sd, su, sdz, ru, rd, rxe, rxu, rxd, cy, cm, ct, op, ope, tm, te, tr,
    shift_s, in_sem, shift_sem, s_sem, r_sem, sb_sem, rb_sem,
):
    es, ed = (es0, es1, es2), (ed0, ed1, ed2)
    e = (es0, ed0, es1, ed1, es2, ed2)
    rb = (rb0, rb1, rb2, rb3, rb4, rb5)
    gx, gy = lax.axis_index("gx"), lax.axis_index("gy")
    ngx, ngy = lax.axis_size("gx"), lax.axis_size("gy")
    core = lax.rem(gx, 2)
    off_gx = lax.rem(gx + 2 * core - 1 + ngx, ngx)
    on_gx = gx + 1 - 2 * core
    up, down = lax.rem(gy + 1, ngy), lax.rem(gy + ngy - 1, ngy)
    rows = (core, 1 - core)

    copies = []
    for r in (0, 1):
        for t, (src, dst) in enumerate(((off_h, off), (occ_h, occ), (pos_h, pos), (th_h, th), (vel_h, vel))):
            view = src.at[:, rows[r]] if t < 2 else src.at[:, :, rows[r]]
            c = pltpu.make_async_copy(view, dst.at[r], in_sem.at[r, t])
            c.start()
            copies.append(c)
        if r == 0:
            shift_copy = pltpu.make_async_copy(shift_h, shift_s, shift_sem)
            shift_copy.start()

    barrier = pltpu.get_barrier_semaphore()
    for to in ((off_gx, gy), (on_gx, gy), (gx, up), (gx, down), (off_gx, up), (off_gx, down), (on_gx, up), (on_gx, down)):
        pl.semaphore_signal(barrier, inc=1, device_id=to, device_id_type=MESH)

    sdz[...] = jnp.zeros_like(sdz)
    su[...] = jnp.zeros_like(su)
    te[...] = jnp.zeros_like(te)
    shift_copy.wait()
    sh = [shift_s[0], shift_s[1], shift_s[2]]

    core_f = core.astype(f32)
    xbit = {(0, 1): 1.0 - core_f, (0, 0): core_f, (1, 1): core_f, (1, 0): 1.0 - core_f}
    flip = (core * 4, (1 - core) * 4)

    def chunked(body):
        def step(t, carry):
            ys = pl.ds(pl.multiple_of(8 * (t // 2), 8), 8)
            zs = pl.ds(pl.multiple_of(128 * lax.rem(t, 2), 128), 128)
            body(ys, zs)
            return carry
        lax.fori_loop(0, 4, step, 0)

    def make_codes(r):
        x = sh[0] ^ flip[r]
        for m in range(SLOTS):
            code[r, m] = jnp.where(occ[r, m] == 1, off[r, m] ^ x, 8)

    def accumulate(acc, mask, vals):
        for f, v in enumerate(vals):
            term = jnp.where(mask, v, 0.0)
            acc[f] = term if acc[f] is None else acc[f] + term

    def static_moments(r, p):
        def body(ys, zs):
            acc = [[None] * STATIC for _ in range(4)]
            for m in range(SLOTS):
                k = code[r, m, ys, zs]
                x, y, z = (pos[r, a, m, ys, zs] for a in range(3))
                vals = [1.0, x, y, z, x * x, y * y, z * z, x * y, x * z, y * z]
                for q in range(4):
                    accumulate(acc[q], k == p * 4 + q, vals)
            for q in range(4):
                for f in range(STATIC):
                    gs[r, p * 4 + q, f, ys, zs] = acc[q][f]
        chunked(body)

    def dynamic_moments(s, r, p):
        def body(ys, zs):
            acc = [[None] * DYNAMIC for _ in range(4)]
            for m in range(SLOTS):
                k = code[r, m, ys, zs]
                x, y, z = (pos[r, a, m, ys, zs] for a in range(3))
                if s == 0:
                    w = [vel[r, a, m, ys, zs] - th[r, a, m, ys, zs] for a in range(3)]
                else:
                    w = [th[r, a, (m + s - 1) % SLOTS, ys, zs] - th[r, a, (m + s) % SLOTS, ys, zs] for a in range(3)]
                vals = w + [y * w[2] - z * w[1], z * w[0] - x * w[2], x * w[1] - y * w[0]]
                for q in range(4):
                    accumulate(acc[q], k == p * 4 + q, vals)
            for q in range(4):
                for f in range(DYNAMIC):
                    gd[s, r, p * 4 + q, f, ys, zs] = acc[q][f]
        chunked(body)

    def static_field(load, f, bx, by, bz):
        v = load(f)
        if f == 1:
            v = v + bx * load(0)
        elif f == 2 and by:
            v = v + load(0)
        elif f == 3 and bz:
            v = v + load(0)
        elif f == 4:
            v = v + bx * (2.0 * load(1) + load(0))
        elif f == 5 and by:
            v = v + (2.0 * load(2) + load(0))
        elif f == 6 and bz:
            v = v + (2.0 * load(3) + load(0))
        elif f == 7:
            v = v + bx * (load(2) + load(0) if by else load(2))
            v = v + load(1) if by else v
        elif f == 8:
            v = v + bx * (load(3) + load(0) if bz else load(3))
            v = v + load(1) if bz else v
        elif f == 9:
            if by:
                v = v + load(3)
            if bz:
                v = v + load(2)
            if by and bz:
                v = v + load(0)
        return v

    def dynamic_field(load, f, bx, by, bz):
        v = load(f)
        if f == 3:
            v = v + load(2) if by else v
            v = v - load(1) if bz else v
        elif f == 4:
            v = v - bx * load(2)
            v = v + load(0) if bz else v
        elif f == 5:
            v = v + bx * load(1)
            v = v - load(0) if by else v
        return v

    not_last = lax.broadcasted_iota(jnp.int32, (16, 256), 0) < 15
    is_last = lax.broadcasted_iota(jnp.int32, (16, 256), 0) == 15
    is_first = lax.broadcasted_iota(jnp.int32, (16, 256), 0) == 0

    def assemble(ph, row, source, field):
        g, base = GROUP[ph], BASE[ph]
        for f in range(FIELDS[ph]):
            planes = []
            for bz in (0, 1):
                total = [None, None]
                for by in (0, 1):
                    for r, p in ROW_PARTS[row]:
                        load = functools.partial(source, r, p * 4 + by * 2 + bz)
                        v = field(load, f, xbit[r, p], by, bz)
                        total[by] = v if total[by] is None else total[by] + v
                sdz[bz, base + f : base + f + 1] = total[1][0:1]
                planes.append(total[0] + jnp.where(not_last, pltpu.roll(total[1], 15, 0), 0.0))
            whole = planes[0] + pltpu.roll(planes[1], 255, 1)
            e[ph][row, f] = whole
            su[g, row, base + f : base + f + 1] = whole[15:16]

    def edges(g, row):
        n = SPAN[g]
        sd[g, row, 0:n] = sdz[0, 0:n] + pltpu.roll(sdz[1, 0:n], 255, 1)

    def remote(src, dst, send, recv, to):
        return pltpu.make_async_remote_copy(
            src_ref=src, dst_ref=dst, send_sem=send, recv_sem=recv, device_id=to, device_id_type=MESH
        )

    def small(g, j, src, dst, to):
        return remote(src, dst, s_sem.at[g, j], r_sem.at[g, j], to)

    def y_messages(g, row):
        fs = pl.ds(0, SPAN[g])
        return [
            small(g, 6 + 2 * row, sd.at[g, row, fs], ru.at[g, row, fs], (gx, down)),
            small(g, 7 + 2 * row, su.at[g, row, fs], rd.at[g, row, fs], (gx, up)),
        ]

    def x_messages(g, row):
        if row == M:
            return []
        fs = pl.ds(0, SPAN[g])
        side, to = (0, off_gx) if row == O else (1, on_gx)
        low, high = sd.at[g, row, fs], su.at[g, row, fs]
        if g == B:
            return [small(g, 3 * side, cy.at[side, fs], rxe.at[g, side, fs], (to, gy))]
        return [
            small(g, 3 * side + 1, low, rxu.at[g, side, fs], (to, down)),
            small(g, 3 * side + 2, high, rxd.at[g, side, fs], (to, up)),
            small(g, 3 * side, low, rxe.at[g, side, fs], (to, gy)),
        ]

    def bulk(ph, row, halves=(0, 1)):
        side, to = (0, off_gx) if row == O else (1, on_gx)
        if row == M:
            return []
        if GROUP[ph] != B:
            return [remote(e[ph].at[row], rb[ph].at[side], sb_sem.at[ph, side, 0], rb_sem.at[ph, side, 0], (to, gy))]
        out = []
        for h in halves:
            cols = pl.ds(8 * h, 8)
            src, dst = e[ph].at[row, :, cols], rb[ph].at[side, :, cols]
            out.append(remote(src, dst, sb_sem.at[ph, side, h], rb_sem.at[ph, side, h], (to, gy)))
        return out

    def start(messages):
        for c in messages:
            c.start()

    def arrive(messages):
        for c in messages:
            c.wait_recv()

    def combine(row):
        side = 0 if row == O else 1
        arrive(y_messages(B, row))
        cy[side] = sd[B, row] + rd[B, row]
        for ph in (2, 4):
            for f in range(STATIC):
                k = BASE[ph] + f
                e[ph][row, f, 8:16] = e[ph][row, f, 8:16] + jnp.where(is_last[8:16], ru[B, row, k : k + 1], 0.0)
        start(x_messages(B, row))

    def totals(g, row):
        n = SPAN[g]
        side = 0 if row == O else 1
        if g != B or row == M:
            arrive(y_messages(g, row))
        arrive(x_messages(g, row))
        if row == M:
            low, high = sd[g, row, 0:n] + rd[g, row, 0:n], ru[g, row, 0:n]
        elif g == B:
            low, high = cy[side] + rxe[g, side], None
        else:
            low = sd[g, row, 0:n] + rd[g, row, 0:n] + rxe[g, side, 0:n] + rxd[g, side, 0:n]
            high = ru[g, row, 0:n] + rxu[g, side, 0:n]
        cm[g, row, 0:n] = low
        if high is not None:
            ct[g, row, 0:n] = high

    def rim(ph, row, f):
        k = BASE[ph] + f
        return cm[GROUP[ph], row, k : k + 1]

    def total(ph, row, f):
        v = e[ph][row, f]
        if row != M:
            v = v + rb[ph][0 if row == O else 1, f]
            if GROUP[ph] == B:
                return v
        k = BASE[ph] + f
        return v + jnp.where(is_last, ct[GROUP[ph], row, k : k + 1], 0.0)

    def invert(a):
        n, sx, sy, sz, xx, yy, zz, xy, xz, yz = a
        inv = 1.0 / jnp.maximum(n, 1.0)
        cx, cy, cz = sx * inv, sy * inv, sz * inv
        mxx, myy, mzz = xx - sx * cx, yy - sy * cy, zz - sz * cz
        kxy, kxz, kyz = sx * cy - xy, sx * cz - xz, sy * cz - yz
        kxx, kyy, kzz = myy + mzz + ridge, mxx + mzz + ridge, mxx + myy + ridge
        axx = kyy * kzz - kyz * kyz
        ayy = kxx * kzz - kxz * kxz
        azz = kxx * kyy - kxy * kxy
        axy = kxz * kyz - kxy * kzz
        axz = kxy * kyz - kxz * kyy
        ayz = kxy * kxz - kxx * kyz
        idet = 1.0 / (kxx * axx + kxy * axy + kxz * axz)
        return [inv, cx, cy, cz, axx * idet, ayy * idet, azz * idet, axy * idet, axz * idet, ayz * idet]

    def respond(o, d):
        inv, cx, cy, cz, axx, ayy, azz, axy, axz, ayz = o
        wx, wy, wz, lx, ly, lz = d
        tx, ty, tz = lx - (cy * wz - cz * wy), ly - (cz * wx - cx * wz), lz - (cx * wy - cy * wx)
        ox = axx * tx + axy * ty + axz * tz
        oy = axy * tx + ayy * ty + ayz * tz
        oz = axz * tx + ayz * ty + azz * tz
        return [wx * inv - (oy * cz - oz * cy), wy * inv - (oz * cx - ox * cz), wz * inv - (ox * cy - oy * cx), ox, oy, oz]

    def static_solve(s, row):
        for f, v in enumerate(invert([total(2 * s, row, f) for f in range(STATIC)])):
            op[row, f] = v
        o = invert([rim(2 * s, row, f) for f in range(STATIC)])
        for f, v in enumerate(o):
            ope[row, f : f + 1] = v

    def dynamic_solve(s, row):
        ph = 2 * s + 1
        t = respond([op[row, f] for f in range(STATIC)], [total(ph, row, f) for f in range(DYNAMIC)])
        x = respond([ope[row, f : f + 1] for f in range(STATIC)], [rim(ph, row, f) for f in range(DYNAMIC)])
        for f in range(DYNAMIC):
            te[row, f : f + 1] = x[f]
            tm[row, f] = t[f]
        te[row, 8:16] = pltpu.roll(te[row, 0:8], 1, 1)
        for f in range(DYNAMIC):
            v = tm[row, f]
            for bz in (0, 1):
                v = v if bz == 0 else pltpu.roll(v, 1, 1)
                tr[row, bz, f] = v
                tr[row, 2 + bz, f] = jnp.where(is_first, te[row, 8 * bz + f : 8 * bz + f + 1], pltpu.roll(v, 1, 0))

    def offset(t, bx, by, bz):
        ax, ay, az, ox, oy, oz = t
        if bz:
            ax, ay = ax + oy, ay - ox
        if by:
            ax, az = ax - oz, az + ox
        return [ax, ay + bx * oz, az - bx * oy, ox, oy, oz]

    def advance(s, r, parts):
        delta = sh[0] ^ sh[s - 1]
        for p in parts:
            row = M if p == 0 else (O if r == 0 else I)
            for q in range(4):
                g = p * 4 + q
                src = g if s == 1 else g ^ delta
                for h in (0, 1):
                    ys = pl.ds(8 * h, 8)
                    t = [tr[row, q, f, ys] for f in range(6)]
                    ax, ay, az, ox, oy, oz = offset(t, xbit[r, p], q // 2, q % 2)
                    n, x, y, z, xx, yy, zz, xy, xz, yz = (gs[r, src, f, ys] for f in range(STATIC))
                    d = [gd[s, r, src, f, ys] for f in range(6)]
                    wb[s - 1, r, g, 0, ys] = d[0] + n * ax + (oy * z - oz * y)
                    wb[s - 1, r, g, 1, ys] = d[1] + n * ay + (oz * x - ox * z)
                    wb[s - 1, r, g, 2, ys] = d[2] + n * az + (ox * y - oy * x)
                    wb[s - 1, r, g, 3, ys] = d[3] + (y * az - z * ay) + ((yy + zz) * ox - xy * oy - xz * oz)
                    wb[s - 1, r, g, 4, ys] = d[4] + (z * ax - x * az) + ((xx + zz) * oy - xy * ox - yz * oz)
                    wb[s - 1, r, g, 5, ys] = d[5] + (x * ay - y * ax) + ((xx + yy) * oz - xz * ox - yz * oy)

    def static_source(s):
        delta = sh[0] ^ sh[s]
        return lambda r, g, f: gs[r, g if s == 0 else g ^ delta, f]

    def dynamic_source(s):
        if s == 0:
            return lambda r, g, f: gd[0, r, g, f]
        delta = sh[s - 1] ^ sh[s]
        return lambda r, g, f: wb[s - 1, r, g ^ delta, f]

    def finish(r, parts):
        delta = sh[0] ^ sh[2]
        def body(ys, zs):
            tables = {}
            for p in parts:
                row = M if p == 0 else (O if r == 0 else I)
                for q in range(4):
                    t = [tr[row, q, f, ys, zs] for f in range(6)]
                    tables[p, q] = offset(t, xbit[r, p], q // 2, q % 2)
            for m in range(SLOTS):
                k = code[r, m, ys, zs] ^ delta
                bz, by, bx = (k & 1) == 1, (k & 2) == 2, (k & 4) == 4
                t = []
                for f in range(6):
                    c = []
                    for p in parts:
                        low = jnp.where(bz, tables[p, 1][f], tables[p, 0][f])
                        c.append(jnp.where(by, jnp.where(bz, tables[p, 3][f], tables[p, 2][f]), low))
                    t.append(c[0] if len(c) == 1 else jnp.where(bx, c[1], c[0]))
                ax, ay, az, ox, oy, oz = t
                x, y, z = (pos[r, a, m, ys, zs] for a in range(3))
                hot = [th[r, a, (m + 2) % SLOTS, ys, zs] for a in range(3)]
                fresh = [hot[0] + ax + (oy * z - oz * y), hot[1] + ay + (oz * x - ox * z), hot[2] + az + (ox * y - oy * x)]
                mine = k < 8 if parts != (1,) else (k & 12) == 4
                for a in range(3):
                    rest = out_ref[a, m, rows[r], ys, zs] if parts == (1,) else 0.0
                    out_ref[a, m, rows[r], ys, zs] = jnp.where(mine, fresh[a], rest)
        chunked(body)

    for t in (0, 1, 2):
        copies[t].wait()
    make_codes(0)
    static_moments(0, 1)
    assemble(0, O, static_source(0), static_field)
    pl.semaphore_wait(barrier, 8)
    start(bulk(0, O))
    for t in (3, 4):
        copies[t].wait()
    dynamic_moments(0, 0, 1)
    assemble(1, O, dynamic_source(0), dynamic_field)
    edges(A, O)
    start(y_messages(A, O) + x_messages(A, O))
    static_moments(0, 0)
    assemble(2, O, static_source(1), static_field)
    assemble(4, O, static_source(2), static_field)
    edges(B, O)
    start(y_messages(B, O) + bulk(1, O))
    for t in range(5, 10):
        copies[t].wait()
    make_codes(1)
    static_moments(1, 1)
    dynamic_moments(0, 1, 1)
    assemble(0, I, static_source(0), static_field)
    assemble(1, I, dynamic_source(0), dynamic_field)
    edges(A, I)
    start(y_messages(A, I) + x_messages(A, I) + bulk(0, I) + bulk(1, I))
    dynamic_moments(0, 0, 0)
    static_moments(1, 0)
    dynamic_moments(0, 1, 0)
    assemble(0, M, static_source(0), static_field)
    assemble(1, M, dynamic_source(0), dynamic_field)
    edges(A, M)
    start(y_messages(A, M) + bulk(2, O, (0,)))
    for row in (I, M):
        assemble(2, row, static_source(1), static_field)
        assemble(4, row, static_source(2), static_field)
        edges(B, row)
        start(y_messages(B, row))
    combine(O)
    start(bulk(2, O, (1,)))
    dynamic_moments(1, 0, 0)
    dynamic_moments(1, 0, 1)
    dynamic_moments(1, 1, 0)
    dynamic_moments(1, 1, 1)
    for s in (0, 1, 2):
        for row in (M, I):
            if s < 2:
                totals((A, B)[s], row)
            arrive(bulk(2 * s, row))
            static_solve(s, row)
            if s > 0:
                totals((C, D)[s - 1], row)
            arrive(bulk(2 * s + 1, row))
            dynamic_solve(s, row)
        if s < 2:
            advance(s + 1, 1, (0, 1))
            assemble(2 * s + 3, I, dynamic_source(s + 1), dynamic_field)
            edges((C, D)[s], I)
            start(y_messages((C, D)[s], I) + x_messages((C, D)[s], I) + bulk(2 * s + 3, I))
            advance(s + 1, 0, (0,))
        else:
            finish(1, (0, 1))
            finish(0, (0,))
        if s < 2:
            totals((A, B)[s], O)
        arrive(bulk(2 * s, O))
        static_solve(s, O)
        if s > 0:
            totals((C, D)[s - 1], O)
        arrive(bulk(2 * s + 1, O))
        dynamic_solve(s, O)
        if s < 2:
            advance(s + 1, 0, (1,))
            for row in (O, M):
                assemble(2 * s + 3, row, dynamic_source(s + 1), dynamic_field)
                edges((C, D)[s], row)
                start(y_messages((C, D)[s], row) + x_messages((C, D)[s], row))
            start(bulk(2 * s + 3, O))
            if s == 0:
                start(bulk(4, O))
                dynamic_moments(2, 0, 0)
                dynamic_moments(2, 0, 1)
                combine(I)
                start(bulk(2, I) + bulk(4, I))
                dynamic_moments(2, 1, 0)
                dynamic_moments(2, 1, 1)
        else:
            finish(0, (1,))
    for row in (O, M, I):
        for g in range(4):
            for c in y_messages(g, row) + x_messages(g, row):
                c.wait_send()
        for ph in range(6):
            for c in bulk(ph, row):
                c.wait_send()


def local(positions, velocities, thermal, offsets, occupancy, shift_codes):
    any_space = pl.BlockSpec(memory_space=pltpu.HBM)
    rim = lambda *lead: pltpu.VMEM((*lead, 24, 256), f32)
    per = lambda *lead: pltpu.VMEM((*lead, 16, 256), f32)
    return pl.pallas_call(
        kernel,
        out_shape=jax.ShapeDtypeStruct(positions.shape, f32),
        in_specs=[any_space] * 6,
        out_specs=pl.BlockSpec(memory_space=pltpu.VMEM),
        scratch_shapes=[
            per(2, 3, SLOTS), per(2, 3, SLOTS), per(2, 3, SLOTS),
            pltpu.VMEM((2, SLOTS, 16, 256), jnp.int32), pltpu.VMEM((2, SLOTS, 16, 256), jnp.int32), pltpu.VMEM((2, SLOTS, 16, 256), jnp.int32),
            per(2, 8, STATIC), per(3, 2, 8, DYNAMIC), per(2, 2, 8, DYNAMIC),
            *[per(3, n) for n in FIELDS],
            *[per(2, n) for n in FIELDS],
            rim(4, 3), rim(4, 3), rim(2), rim(4, 3), rim(4, 3), rim(4, 2), rim(4, 2), rim(4, 2), rim(2), rim(4, 3), rim(4, 3),
            per(3, STATIC), per(3), per(3, DYNAMIC), per(3), per(3, 4, DYNAMIC),
            pltpu.SMEM((3,), jnp.int32), pltpu.SemaphoreType.DMA((2, 5)), pltpu.SemaphoreType.DMA,
            pltpu.SemaphoreType.DMA((4, 12)), pltpu.SemaphoreType.DMA((4, 12)),
            pltpu.SemaphoreType.DMA((6, 2, 2)), pltpu.SemaphoreType.DMA((6, 2, 2)),
        ],
        compiler_params=pltpu.CompilerParams(
            collective_id=0, has_side_effects=True, vmem_limit_bytes=40 * 1024 * 1024
        ),
    )(*(pltpu.with_memory_space_constraint(v, pltpu.HBM) for v in (shift_codes, positions, velocities, thermal, offsets, occupancy)))


def solution(mesh):
    in_specs = (
        P(None, None, "gx", "gy", None),
        P(None, None, "gx", "gy", None),
        P(None, None, "gx", "gy", None),
        P(None, "gx", "gy", None),
        P(None, "gx", "gy", None),
        P(),
    )
    out_specs = P(None, None, "gx", "gy", None)
    return jax.shard_map(local, mesh=mesh, in_specs=in_specs, out_specs=out_specs, check_vma=False)
```

```python
import functools

import jax
import jax.numpy as jnp
from jax import lax
from jax.experimental import pallas as pl
from jax.experimental.pallas import tpu as pltpu
from jax.sharding import PartitionSpec as P

MESH = pl.DeviceIdType.MESH
f32 = jnp.float32
SLOTS = 12
ridge = 0.5

O, M, I = 0, 1, 2
ROW_PARTS = {O: ((0, 1),), M: ((0, 0), (1, 0)), I: ((1, 1),)}
STATIC, DYNAMIC = 10, 6
FIELDS = (STATIC, DYNAMIC) * 3
A, B, C, E, D = 0, 1, 2, 3, 4
GROUP = (A, A, B, C, E, D)
BASE = (0, STATIC, 0, 0, 0, 0)
SPAN = (16, 16, 8, 16, 8)


def kernel(
    shift_h, pos_h, vel_h, th_h, off_h, occ_h, out_ref,
    pos, vel, th, off, occ, code, gs, gd, wb,
    es0, ed0, es1, ed1, es2, ed2,
    rb0, rb1, rb2, rb3, rb4, rb5,
    sd, su, sdz, ry, rx, everything, cy, cm, ct, op, ope, tm, te, tr,
    shift_s, in_sem, shift_sem, s_sem, r_sem, rb_sem,
):
    es, ed = (es0, es1, es2), (ed0, ed1, ed2)
    e = (es0, ed0, es1, ed1, es2, ed2)
    rb = (rb0, rb1, rb2, rb3, rb4, rb5)
    gx, gy = lax.axis_index("gx"), lax.axis_index("gy")
    ngx, ngy = lax.axis_size("gx"), lax.axis_size("gy")
    core = lax.rem(gx, 2)
    off_gx = lax.rem(gx + 2 * core - 1 + ngx, ngx)
    on_gx = gx + 1 - 2 * core
    up, down = lax.rem(gy + 1, ngy), lax.rem(gy + ngy - 1, ngy)
    rows = (core, 1 - core)

    copies = []
    for r in (0, 1):
        for t, (src, dst) in enumerate(((off_h, off), (occ_h, occ), (pos_h, pos), (th_h, th), (vel_h, vel))):
            view = src.at[:, rows[r]] if t < 2 else src.at[:, :, rows[r]]
            c = pltpu.make_async_copy(view, dst.at[r], in_sem.at[r, t])
            c.start()
            copies.append(c)
        if r == 0:
            shift_copy = pltpu.make_async_copy(shift_h, shift_s, shift_sem)
            shift_copy.start()

    barrier = pltpu.get_barrier_semaphore()
    for to in ((off_gx, gy), (on_gx, gy), (gx, up), (gx, down), (off_gx, up), (off_gx, down), (on_gx, up), (on_gx, down)):
        pl.semaphore_signal(barrier, inc=1, device_id=to, device_id_type=MESH)

    sdz[...] = jnp.zeros_like(sdz)
    su[...] = jnp.zeros_like(su)
    te[...] = jnp.zeros_like(te)
    shift_copy.wait()
    sh = [shift_s[0], shift_s[1], shift_s[2]]

    core_f = core.astype(f32)
    xbit = {(0, 1): 1.0 - core_f, (0, 0): core_f, (1, 1): core_f, (1, 0): 1.0 - core_f}
    flip = (core * 4, (1 - core) * 4)

    def chunked(body):
        def step(t, carry):
            ys = pl.ds(pl.multiple_of(8 * (t // 2), 8), 8)
            zs = pl.ds(pl.multiple_of(128 * lax.rem(t, 2), 128), 128)
            body(ys, zs)
            return carry
        lax.fori_loop(0, 4, step, 0)

    def make_codes(r):
        x = sh[0] ^ flip[r]
        for m in range(SLOTS):
            code[r, m] = jnp.where(occ[r, m] == 1, off[r, m] ^ x, 8)

    def accumulate(acc, mask, vals):
        for f, v in enumerate(vals):
            term = jnp.where(mask, v, 0.0)
            acc[f] = term if acc[f] is None else acc[f] + term

    def static_moments(r, p):
        def body(ys, zs):
            acc = [[None] * STATIC for _ in range(4)]
            for m in range(SLOTS):
                k = code[r, m, ys, zs]
                x, y, z = (pos[r, a, m, ys, zs] for a in range(3))
                vals = [1.0, x, y, z, x * x, y * y, z * z, x * y, x * z, y * z]
                for q in range(4):
                    accumulate(acc[q], k == p * 4 + q, vals)
            for q in range(4):
                for f in range(STATIC):
                    gs[r, p * 4 + q, f, ys, zs] = acc[q][f]
        chunked(body)

    def dynamic_moments(s, r, p):
        def body(ys, zs):
            acc = [[None] * DYNAMIC for _ in range(4)]
            for m in range(SLOTS):
                k = code[r, m, ys, zs]
                x, y, z = (pos[r, a, m, ys, zs] for a in range(3))
                if s == 0:
                    w = [vel[r, a, m, ys, zs] - th[r, a, m, ys, zs] for a in range(3)]
                else:
                    w = [th[r, a, (m + s - 1) % SLOTS, ys, zs] - th[r, a, (m + s) % SLOTS, ys, zs] for a in range(3)]
                vals = w + [y * w[2] - z * w[1], z * w[0] - x * w[2], x * w[1] - y * w[0]]
                for q in range(4):
                    accumulate(acc[q], k == p * 4 + q, vals)
            for q in range(4):
                for f in range(DYNAMIC):
                    gd[s, r, p * 4 + q, f, ys, zs] = acc[q][f]
        chunked(body)

    def static_field(load, f, bx, by, bz):
        v = load(f)
        if f == 1:
            v = v + bx * load(0)
        elif f == 2 and by:
            v = v + load(0)
        elif f == 3 and bz:
            v = v + load(0)
        elif f == 4:
            v = v + bx * (2.0 * load(1) + load(0))
        elif f == 5 and by:
            v = v + (2.0 * load(2) + load(0))
        elif f == 6 and bz:
            v = v + (2.0 * load(3) + load(0))
        elif f == 7:
            v = v + bx * (load(2) + load(0) if by else load(2))
            v = v + load(1) if by else v
        elif f == 8:
            v = v + bx * (load(3) + load(0) if bz else load(3))
            v = v + load(1) if bz else v
        elif f == 9:
            if by:
                v = v + load(3)
            if bz:
                v = v + load(2)
            if by and bz:
                v = v + load(0)
        return v

    def dynamic_field(load, f, bx, by, bz):
        v = load(f)
        if f == 3:
            v = v + load(2) if by else v
            v = v - load(1) if bz else v
        elif f == 4:
            v = v - bx * load(2)
            v = v + load(0) if bz else v
        elif f == 5:
            v = v + bx * load(1)
            v = v - load(0) if by else v
        return v

    not_last = lax.broadcasted_iota(jnp.int32, (16, 256), 0) < 15
    is_last = lax.broadcasted_iota(jnp.int32, (16, 256), 0) == 15
    is_first = lax.broadcasted_iota(jnp.int32, (16, 256), 0) == 0

    def assemble(ph, row, source, field):
        g, base = GROUP[ph], BASE[ph]
        for f in range(FIELDS[ph]):
            planes = []
            for bz in (0, 1):
                total = [None, None]
                for by in (0, 1):
                    for r, p in ROW_PARTS[row]:
                        load = functools.partial(source, r, p * 4 + by * 2 + bz)
                        v = field(load, f, xbit[r, p], by, bz)
                        total[by] = v if total[by] is None else total[by] + v
                sdz[bz, base + f : base + f + 1] = total[1][0:1]
                planes.append(total[0] + jnp.where(not_last, pltpu.roll(total[1], 15, 0), 0.0))
            whole = planes[0] + pltpu.roll(planes[1], 255, 1)
            e[ph][row, f] = whole
            su[g, row, base + f : base + f + 1] = whole[15:16]

    def edges(g, row):
        n = SPAN[g]
        sd[g, row, 0:n] = sdz[0, 0:n] + pltpu.roll(sdz[1, 0:n], 255, 1)

    def remote(src, dst, send, recv, to):
        return pltpu.make_async_remote_copy(
            src_ref=src, dst_ref=dst, send_sem=send, recv_sem=recv, device_id=to, device_id_type=MESH
        )

    def small(g, j, src, dst, to):
        return remote(src, dst, s_sem, r_sem.at[g, j], to)

    def y_messages(g, row):
        fs = pl.ds(0, SPAN[g])
        return [
            small(g, row, sd.at[g, row, fs], ry.at[g, row, 0, fs], (gx, down)),
            small(g, row, su.at[g, row, fs], ry.at[g, row, 1, fs], (gx, up)),
        ]

    def x_messages(g, row):
        if row == M:
            return []
        fs = pl.ds(0, SPAN[g])
        side, to = (0, off_gx) if row == O else (1, on_gx)
        low, high = sd.at[g, row, fs], su.at[g, row, fs]
        if g == B:
            return [small(g, 3 + side, cy.at[side, fs], rx.at[g, side, 0, fs], (to, gy))]
        return [
            small(g, 3 + side, low, rx.at[g, side, 1, fs], (to, down)),
            small(g, 3 + side, high, rx.at[g, side, 2, fs], (to, up)),
            small(g, 3 + side, low, rx.at[g, side, 0, fs], (to, gy)),
        ]

    def bulk(ph, row, halves=(0, 1)):
        side, to = (0, off_gx) if row == O else (1, on_gx)
        if row == M:
            return []
        if GROUP[ph] != B:
            return [remote(e[ph].at[row], rb[ph].at[side], s_sem, rb_sem.at[ph, side], (to, gy))]
        out = []
        for h in halves:
            cols = pl.ds(8 * h, 8)
            src, dst = e[ph].at[row, :, cols], rb[ph].at[side, :, cols]
            out.append(remote(src, dst, s_sem, rb_sem.at[ph, side], (to, gy)))
        return out

    def start(messages):
        for c in messages:
            c.start()

    def arrive_y(g, row):
        view = ry.at[g, row, :, pl.ds(0, SPAN[g])]
        remote(view, view, s_sem, r_sem.at[g, row], (gx, up)).wait_recv()

    def arrive_x(g, row):
        side = 0 if row == O else 1
        if row != M:
            view = rx.at[g, side, pl.ds(0, 1 if g == B else 3), pl.ds(0, SPAN[g])]
            remote(view, view, s_sem, r_sem.at[g, 3 + side], (gx, up)).wait_recv()

    def arrive_bulk(ph, row):
        side = 0 if row == O else 1
        if row != M:
            view = rb[ph].at[side]
            remote(view, view, s_sem, rb_sem.at[ph, side], (gx, up)).wait_recv()

    def combine(row):
        side = 0 if row == O else 1
        arrive_y(B, row)
        cy[side] = sd[B, row] + ry[B, row, 1]
        for f in range(STATIC):
            e[2][row, f, 8:16] = e[2][row, f, 8:16] + jnp.where(is_last[8:16], ry[B, row, 0, f : f + 1], 0.0)
        start(x_messages(B, row))

    def totals(g, row):
        n = SPAN[g]
        side = 0 if row == O else 1
        if g != B or row == M:
            arrive_y(g, row)
        arrive_x(g, row)
        if row == M:
            low, high = sd[g, row, 0:n] + ry[g, row, 1, 0:n], ry[g, row, 0, 0:n]
        elif g == B:
            low, high = cy[side] + rx[g, side, 0], None
        else:
            low = sd[g, row, 0:n] + ry[g, row, 1, 0:n] + rx[g, side, 0, 0:n] + rx[g, side, 2, 0:n]
            high = ry[g, row, 0, 0:n] + rx[g, side, 1, 0:n]
        cm[g, row, 0:n] = low
        if high is not None:
            ct[g, row, 0:n] = high

    def rim(ph, row, f):
        k = BASE[ph] + f
        return cm[GROUP[ph], row, k : k + 1]

    def total(ph, row, f):
        v = e[ph][row, f]
        if row != M:
            v = v + rb[ph][0 if row == O else 1, f]
            if GROUP[ph] == B:
                return v
        k = BASE[ph] + f
        return v + jnp.where(is_last, ct[GROUP[ph], row, k : k + 1], 0.0)

    def invert(a):
        n, sx, sy, sz, xx, yy, zz, xy, xz, yz = a
        inv = 1.0 / jnp.maximum(n, 1.0)
        cx, cy, cz = sx * inv, sy * inv, sz * inv
        mxx, myy, mzz = xx - sx * cx, yy - sy * cy, zz - sz * cz
        kxy, kxz, kyz = sx * cy - xy, sx * cz - xz, sy * cz - yz
        kxx, kyy, kzz = myy + mzz + ridge, mxx + mzz + ridge, mxx + myy + ridge
        axx = kyy * kzz - kyz * kyz
        ayy = kxx * kzz - kxz * kxz
        azz = kxx * kyy - kxy * kxy
        axy = kxz * kyz - kxy * kzz
        axz = kxy * kyz - kxz * kyy
        ayz = kxy * kxz - kxx * kyz
        idet = 1.0 / (kxx * axx + kxy * axy + kxz * axz)
        return [inv, cx, cy, cz, axx * idet, ayy * idet, azz * idet, axy * idet, axz * idet, ayz * idet]

    def respond(o, d):
        inv, cx, cy, cz, axx, ayy, azz, axy, axz, ayz = o
        wx, wy, wz, lx, ly, lz = d
        tx, ty, tz = lx - (cy * wz - cz * wy), ly - (cz * wx - cx * wz), lz - (cx * wy - cy * wx)
        ox = axx * tx + axy * ty + axz * tz
        oy = axy * tx + ayy * ty + ayz * tz
        oz = axz * tx + ayz * ty + azz * tz
        return [wx * inv - (oy * cz - oz * cy), wy * inv - (oz * cx - ox * cz), wz * inv - (ox * cy - oy * cx), ox, oy, oz]

    def static_solve(s, row):
        for f, v in enumerate(invert([total(2 * s, row, f) for f in range(STATIC)])):
            op[row, f] = v
        o = invert([rim(2 * s, row, f) for f in range(STATIC)])
        for f, v in enumerate(o):
            ope[row, f : f + 1] = v

    def dynamic_solve(s, row):
        ph = 2 * s + 1
        t = respond([op[row, f] for f in range(STATIC)], [total(ph, row, f) for f in range(DYNAMIC)])
        x = respond([ope[row, f : f + 1] for f in range(STATIC)], [rim(ph, row, f) for f in range(DYNAMIC)])
        for f in range(DYNAMIC):
            te[row, f : f + 1] = x[f]
            tm[row, f] = t[f]
        te[row, 8:16] = pltpu.roll(te[row, 0:8], 1, 1)
        for f in range(DYNAMIC):
            v = tm[row, f]
            for bz in (0, 1):
                v = v if bz == 0 else pltpu.roll(v, 1, 1)
                tr[row, bz, f] = v
                tr[row, 2 + bz, f] = jnp.where(is_first, te[row, 8 * bz + f : 8 * bz + f + 1], pltpu.roll(v, 1, 0))

    def offset(t, bx, by, bz):
        ax, ay, az, ox, oy, oz = t
        if bz:
            ax, ay = ax + oy, ay - ox
        if by:
            ax, az = ax - oz, az + ox
        return [ax, ay + bx * oz, az - bx * oy, ox, oy, oz]

    def advance(s, r, parts):
        delta = sh[0] ^ sh[s - 1]
        for p in parts:
            row = M if p == 0 else (O if r == 0 else I)
            for q in range(4):
                g = p * 4 + q
                src = g if s == 1 else g ^ delta
                for h in (0, 1):
                    ys = pl.ds(8 * h, 8)
                    t = [tr[row, q, f, ys] for f in range(6)]
                    ax, ay, az, ox, oy, oz = offset(t, xbit[r, p], q // 2, q % 2)
                    n, x, y, z, xx, yy, zz, xy, xz, yz = (gs[r, src, f, ys] for f in range(STATIC))
                    d = [gd[s, r, src, f, ys] for f in range(6)]
                    wb[s - 1, r, g, 0, ys] = d[0] + n * ax + (oy * z - oz * y)
                    wb[s - 1, r, g, 1, ys] = d[1] + n * ay + (oz * x - ox * z)
                    wb[s - 1, r, g, 2, ys] = d[2] + n * az + (ox * y - oy * x)
                    wb[s - 1, r, g, 3, ys] = d[3] + (y * az - z * ay) + ((yy + zz) * ox - xy * oy - xz * oz)
                    wb[s - 1, r, g, 4, ys] = d[4] + (z * ax - x * az) + ((xx + zz) * oy - xy * ox - yz * oz)
                    wb[s - 1, r, g, 5, ys] = d[5] + (x * ay - y * ax) + ((xx + yy) * oz - xz * ox - yz * oy)

    def static_source(s):
        delta = sh[0] ^ sh[s]
        return lambda r, g, f: gs[r, g if s == 0 else g ^ delta, f]

    def dynamic_source(s):
        if s == 0:
            return lambda r, g, f: gd[0, r, g, f]
        delta = sh[s - 1] ^ sh[s]
        return lambda r, g, f: wb[s - 1, r, g ^ delta, f]

    def finish(r, parts):
        delta = sh[0] ^ sh[2]
        def body(ys, zs):
            tables = {}
            for p in parts:
                row = M if p == 0 else (O if r == 0 else I)
                for q in range(4):
                    t = [tr[row, q, f, ys, zs] for f in range(6)]
                    tables[p, q] = offset(t, xbit[r, p], q // 2, q % 2)
            for m in range(SLOTS):
                k = code[r, m, ys, zs] ^ delta
                bz, by, bx = (k & 1) == 1, (k & 2) == 2, (k & 4) == 4
                t = []
                for f in range(6):
                    c = []
                    for p in parts:
                        low = jnp.where(bz, tables[p, 1][f], tables[p, 0][f])
                        c.append(jnp.where(by, jnp.where(bz, tables[p, 3][f], tables[p, 2][f]), low))
                    t.append(c[0] if len(c) == 1 else jnp.where(bx, c[1], c[0]))
                ax, ay, az, ox, oy, oz = t
                x, y, z = (pos[r, a, m, ys, zs] for a in range(3))
                hot = [th[r, a, (m + 2) % SLOTS, ys, zs] for a in range(3)]
                fresh = [hot[0] + ax + (oy * z - oz * y), hot[1] + ay + (oz * x - ox * z), hot[2] + az + (ox * y - oy * x)]
                mine = k < 8 if parts != (1,) else (k & 12) == 4
                for a in range(3):
                    rest = out_ref[a, m, rows[r], ys, zs] if parts == (1,) else 0.0
                    out_ref[a, m, rows[r], ys, zs] = jnp.where(mine, fresh[a], rest)
        chunked(body)

    for t in (0, 1, 2):
        copies[t].wait()
    make_codes(0)
    static_moments(0, 1)
    assemble(0, O, static_source(0), static_field)
    pl.semaphore_wait(barrier, 8)
    start(bulk(0, O))
    for t in (3, 4):
        copies[t].wait()
    dynamic_moments(0, 0, 1)
    assemble(1, O, dynamic_source(0), dynamic_field)
    edges(A, O)
    start(y_messages(A, O) + x_messages(A, O))
    static_moments(0, 0)
    assemble(2, O, static_source(1), static_field)
    edges(B, O)
    start(y_messages(B, O) + bulk(1, O))
    for t in range(5, 10):
        copies[t].wait()
    make_codes(1)
    static_moments(1, 1)
    dynamic_moments(0, 1, 1)
    assemble(0, I, static_source(0), static_field)
    assemble(1, I, dynamic_source(0), dynamic_field)
    edges(A, I)
    start(y_messages(A, I) + x_messages(A, I) + bulk(0, I) + bulk(1, I))
    dynamic_moments(0, 0, 0)
    static_moments(1, 0)
    dynamic_moments(0, 1, 0)
    assemble(0, M, static_source(0), static_field)
    assemble(1, M, dynamic_source(0), dynamic_field)
    edges(A, M)
    start(y_messages(A, M) + bulk(2, O, (0,)))
    for row in (I, M):
        assemble(2, row, static_source(1), static_field)
        edges(B, row)
        start(y_messages(B, row))
    combine(O)
    start(bulk(2, O, (1,)))
    for row in (O, M, I):
        assemble(4, row, static_source(2), static_field)
        edges(E, row)
    dynamic_moments(1, 0, 0)
    dynamic_moments(1, 0, 1)
    dynamic_moments(1, 1, 0)
    dynamic_moments(1, 1, 1)
    for s in (0, 1, 2):
        for row in (M, I):
            totals((A, B, E)[s], row)
            arrive_bulk(2 * s, row)
            static_solve(s, row)
            if s > 0:
                totals((C, D)[s - 1], row)
            arrive_bulk(2 * s + 1, row)
            dynamic_solve(s, row)
        if s < 2:
            advance(s + 1, 1, (0, 1))
            assemble(2 * s + 3, I, dynamic_source(s + 1), dynamic_field)
            edges((C, D)[s], I)
            start(y_messages((C, D)[s], I) + x_messages((C, D)[s], I) + bulk(2 * s + 3, I))
            advance(s + 1, 0, (0,))
        else:
            finish(1, (0, 1))
            finish(0, (0,))
        totals((A, B, E)[s], O)
        arrive_bulk(2 * s, O)
        static_solve(s, O)
        if s > 0:
            totals((C, D)[s - 1], O)
        arrive_bulk(2 * s + 1, O)
        dynamic_solve(s, O)
        if s < 2:
            advance(s + 1, 0, (1,))
            for row in (O, M):
                assemble(2 * s + 3, row, dynamic_source(s + 1), dynamic_field)
                edges((C, D)[s], row)
                start(y_messages((C, D)[s], row) + x_messages((C, D)[s], row))
            start(bulk(2 * s + 3, O))
            if s == 0:
                dynamic_moments(2, 0, 0)
                dynamic_moments(2, 0, 1)
                combine(I)
                start(bulk(2, I))
                start(y_messages(E, I) + x_messages(E, I) + bulk(4, I))
                dynamic_moments(2, 1, 0)
                dynamic_moments(2, 1, 1)
                for row in (M, O):
                    start(y_messages(E, row) + x_messages(E, row))
                start(bulk(4, O))
        else:
            finish(0, (1,))
    remote(everything, everything, s_sem, r_sem.at[0, 0], (gx, up)).wait_send()


def local(positions, velocities, thermal, offsets, occupancy, shift_codes):
    any_space = pl.BlockSpec(memory_space=pltpu.HBM)
    per = rim = lambda *lead: pltpu.VMEM((*lead, 16, 256), f32)
    return pl.pallas_call(
        kernel,
        out_shape=jax.ShapeDtypeStruct(positions.shape, f32),
        in_specs=[any_space] * 6,
        out_specs=pl.BlockSpec(memory_space=pltpu.VMEM),
        scratch_shapes=[
            per(2, 3, SLOTS), per(2, 3, SLOTS), per(2, 3, SLOTS),
            pltpu.VMEM((2, SLOTS, 16, 256), jnp.int32), pltpu.VMEM((2, SLOTS, 16, 256), jnp.int32), pltpu.VMEM((2, SLOTS, 16, 256), jnp.int32),
            per(2, 8, STATIC), per(3, 2, 8, DYNAMIC), per(2, 2, 8, DYNAMIC),
            *[per(3, n) for n in FIELDS],
            *[per(2, n) for n in FIELDS],
            rim(5, 3), rim(5, 3), rim(2), rim(5, 3, 2), rim(5, 2, 3), rim(140), rim(2), rim(5, 3), rim(5, 3),
            per(3, STATIC), per(3), per(3, DYNAMIC), per(3), per(3, 4, DYNAMIC),
            pltpu.SMEM((3,), jnp.int32), pltpu.SemaphoreType.DMA((2, 5)), pltpu.SemaphoreType.DMA,
            pltpu.SemaphoreType.DMA, pltpu.SemaphoreType.DMA((5, 5)), pltpu.SemaphoreType.DMA((6, 2)),
        ],
        compiler_params=pltpu.CompilerParams(
            collective_id=0, has_side_effects=True, vmem_limit_bytes=40 * 1024 * 1024
        ),
    )(*(pltpu.with_memory_space_constraint(v, pltpu.HBM) for v in (shift_codes, positions, velocities, thermal, offsets, occupancy)))


def solution(mesh):
    in_specs = (
        P(None, None, "gx", "gy", None),
        P(None, None, "gx", "gy", None),
        P(None, None, "gx", "gy", None),
        P(None, "gx", "gy", None),
        P(None, "gx", "gy", None),
        P(),
    )
    out_specs = P(None, None, "gx", "gy", None)
    return jax.shard_map(local, mesh=mesh, in_specs=in_specs, out_specs=out_specs, check_vma=False)
```
